32 devices in a mesh: member: 2 (over x), lat: 16 (over z, y, core).
Axes of the slice: x: 2, y: 2, z: 4, core: 2. Of those that a mesh axis runs over, the one named last changes fastest.
Arguments:
- field: bfloat16 [192, 1440, 256], P(('member', 'lat')), parts along dimension 0, may hold values from -3000 to 3000
- gain: float32 [256], replicated, may hold values from 0.1 to 1.9
- slot_wave: int32 [96], replicated, may hold values from 0 to 96, as said below
- legendre: bfloat16 [96, 96, 96], P('lat'), may hold values from -0.625 to 0.625
- mixing: bfloat16 [96, 2, 256, 256], P('lat'), may hold values from -0.25 to 0.25
Outputs:
- result: bfloat16 [192, 1440, 256], P(('member', 'lat')), parts along dimension 0
The draws below stay inside these ranges and needn't reach their ends.
There are 2 independent parts, one for each index of `member`. The reference program is written for one: setup_inputs(seed, part) draws one part's arguments, and reference() takes and returns one part's arrays. A program takes and returns all parts, laid end to end along the dimension named above; an argument that names none is the same for every part. Nothing has to cross between parts.
Inputs may be any that keep to these rules, and one draw needn't show every extreme that they name: `slot_wave`: each wavenumber 0 to 95 stands in exactly one slot and every other slot holds 96; slots 2k and 2k+1 of one lat index hold wavenumbers adding up to (4k+2)16 - 1 where both are below 96.
All inputs are finite; a program needn't handle non-finite values.
Results may differ from the reference program's by a relative error of at most 0.0085.
Values may be sent and summed in bfloat16 or wider, within the bound.
No kernel may reach another device: no remote copies, remote signals or barrier semaphores. Data moves between devices by JAX's collectives and lax.ppermute only.
A program may use at most 64 MiB of HBM per device.

```python
import math
import jax
import jax.numpy as jnp
from jax import lax

C = 256
NLON = 1440
NLAT = 96
DEG = 96
SLOT_DEV = 6
SLOTS = 96
N_LAT = 16


def draw_field(key, part):
    keys = jax.random.split(key, 3)
    rows = jnp.arange(NLAT, dtype=jnp.float32) / NLAT
    wobble = 0.3 * jax.random.normal(keys[0], (NLAT,), jnp.float32)
    chan = 10.0 ** jax.random.uniform(keys[1], (C,), jnp.float32, 0.0, 1.0)
    base = jnp.clip(jax.random.normal(keys[2], (NLAT, NLON, C), jnp.float32), -6.0, 6.0)
    row_exp = rows + wobble
    row_exp = jnp.clip(row_exp, -0.5, 1.5)
    values = base * (10.0 ** row_exp)[:, None, None] * chan[None, None, :]
    return values.astype(jnp.bfloat16)


def draw_slot_wave(key, part):
    rounds = SLOT_DEV
    pairs = (rounds + 1) // 2
    keys = jax.random.split(jax.random.fold_in(key, 17), pairs)
    perms = jax.vmap(lambda k: jax.random.permutation(k, N_LAT))(keys)
    round_ids = jnp.arange(rounds, dtype=jnp.int32)[:, None]
    places = jnp.arange(N_LAT, dtype=jnp.int32)[None, :]
    chosen = perms[round_ids[:, 0] // 2]
    picks = jnp.where(round_ids % 2 == 0, places, N_LAT - 1 - places)
    owner = jnp.take_along_axis(chosen, jnp.broadcast_to(picks, (rounds, N_LAT)), axis=1)
    wave = round_ids * N_LAT + places
    wave = jnp.where(wave < DEG, wave, DEG)
    slot = owner * SLOT_DEV + round_ids
    table = jnp.zeros((SLOTS,), jnp.int32)
    return table.at[slot.reshape(-1)].set(jnp.broadcast_to(wave, (rounds, N_LAT)).reshape(-1).astype(jnp.int32))


def levels(rng, dims, cuts, smallest, high):
    level, own = 1.0, jax.random.fold_in(rng, 6)
    for dim, shards_of in cuts:
        heights = jnp.exp(jax.random.uniform(jax.random.fold_in(own, dim), (shards_of,), jnp.float32, smallest / len(cuts), high / len(cuts)))
        level = level * jnp.repeat(heights, dims[dim] // shards_of).reshape([-1 if axis == dim else 1 for axis in range(len(dims))])
    return level


def noise(key, shape, scale, reach, cuts=(), kind=jnp.bfloat16):
    result = jax.random.normal(key, shape, jnp.float32) * scale
    if len(cuts) > 0:
        result = levels(key, shape, cuts, -0.22, 0.18) * result
    return jnp.clip(result, min=-reach, max=reach).astype(kind)


def setup_inputs(seed: int = 0, part: int = 0) -> dict:
    key_of = jax.random.split(jax.random.key(seed), 6)
    part_keys = jax.random.split(jax.random.fold_in(key_of[5], part), 6)
    field = draw_field(jax.random.fold_in(jax.random.fold_in(key_of[5], part), 71), part)
    gain = jnp.clip(1.0 + 0.18 * jax.random.normal(key_of[1], (C,), jnp.float32), 0.1, 1.9)
    slot_wave = draw_slot_wave(jax.random.fold_in(key_of[5], 71), part)
    legendre = noise(key_of[3], (SLOTS, DEG, NLAT), NLAT ** -0.5, 0.625, ((0, 16),))
    mixing = noise(key_of[4], (SLOTS, 2, C, C), (2 * C) ** -0.5, 0.25, ((0, 16),))
    return {"field": field, "gain": gain, "slot_wave": slot_wave, "legendre": legendre, "mixing": mixing}


def phase_tables(waves, width):
    points = jnp.arange(width, dtype=jnp.int32)
    phase = (waves[:, None] * points[None, :] % width).astype(jnp.float32) * (2.0 * math.pi / width)
    return (jnp.cos(phase), jnp.sin(phase))

def block_weight(mixing):
    real_part = mixing[:, 0]
    imag_part = mixing[:, 1]
    upper = jnp.concatenate([real_part, imag_part], axis=2)
    lower = jnp.concatenate([-imag_part, real_part], axis=2)
    return jnp.concatenate([upper, lower], axis=1)

def reference(field, gain, slot_wave, legendre, mixing):
    values = field.astype(jnp.float32)
    mean = lax.optimization_barrier(jnp.mean(values, axis=(0, 1)))
    var = lax.optimization_barrier(jnp.mean((values - mean) ** 2, axis=(0, 1)))
    normed = ((values - mean) * (gain / jnp.sqrt(var + 1e-05))).astype(jnp.bfloat16)
    cosine, sine = phase_tables(slot_wave, NLON)
    forward = jnp.stack([cosine, -sine]).astype(jnp.bfloat16)
    weight_m = jnp.where(slot_wave == 0, 1.0, 2.0).astype(jnp.float32)[:, None]
    inverse = jnp.stack([weight_m * cosine, -weight_m * sine]).astype(jnp.bfloat16)
    inv_root = 1.0 / math.sqrt(NLON)
    spectrum = jnp.einsum('anc,rkn->karc', normed.astype(jnp.float32), forward.astype(jnp.float32)) * inv_root
    spectrum = spectrum.astype(jnp.bfloat16).reshape(SLOTS, NLAT, 2 * C)
    big = block_weight(mixing)
    lat_scale = math.sqrt(NLAT / DEG)
    degrees = jnp.arange(DEG, dtype=jnp.int32)

    def one_slot(items):
        table, spec, weight, wave = items
        coef = jnp.dot(table, spec, preferred_element_type=jnp.float32)
        coef = jnp.where((degrees >= wave)[:, None], coef, 0.0).astype(jnp.bfloat16)
        mixed = jnp.dot(coef, weight, preferred_element_type=jnp.float32).astype(jnp.bfloat16)
        back = jnp.dot(table.T, mixed, preferred_element_type=jnp.float32) * lat_scale
        return back.astype(jnp.bfloat16)
    back = lax.map(one_slot, (legendre, spectrum, big, slot_wave))
    back = back.reshape(SLOTS, NLAT, 2, C)
    filtered = jnp.einsum('karc,rkn->anc', back.astype(jnp.float32), inverse.astype(jnp.float32)) * inv_root
    return (normed.astype(jnp.float32) + filtered).astype(jnp.bfloat16)
```

```python
import functools
import math

import jax
import jax.numpy as jnp
import numpy as np
from jax import lax
from jax.experimental import pallas as pl
from jax.experimental.pallas import tpu as pltpu
from jax.sharding import PartitionSpec as P

F32 = jnp.float32
BF16 = jnp.bfloat16
PIECES = 3
EXTRA = 16


def dot(a, b, dims=((1,), (0,))):
    return lax.dot_general(a, b, (dims, ((), ())), preferred_element_type=F32)


def wave_tables(degs, width):
    turns = np.outer(np.arange(degs), np.arange(width)) % width
    phase = turns.astype(np.float64) * (2.0 * math.pi / width)
    table = np.concatenate([np.cos(phase), -np.sin(phase)]).astype(BF16)
    return table, table.astype(np.float64).sum(axis=1).astype(np.float32)


def forward_kernel(field, table, sums, column, payload, spec, packed, first, acc):
    step = pl.program_id(0)
    steps, rows, chans = spec.shape
    degs = rows // 2
    width = field.shape[1]
    block = field[0]

    @pl.when(step == 0)
    def _():
        first[...] = jnp.broadcast_to(block[0:1].astype(F32), first.shape)
        acc[...] = jnp.zeros_like(acc)

    spec[step] = dot(table[...], block)
    shifted = block.astype(F32).reshape(width // 8, 8, chans) - first[...]
    acc[0] += jnp.sum(shifted, axis=0)
    acc[1] += jnp.sum(shifted * shifted, axis=0)

    @pl.when(step == steps - 1)
    def _():
        count = float(steps * width)
        shift = jnp.sum(acc[0], axis=0, keepdims=True) / count
        square = jnp.sum(acc[1], axis=0, keepdims=True)
        mean = first[0:1] + shift
        spread = jnp.maximum(square - count * shift * shift, 0.0)
        for a in range(steps):
            centred = (spec[a] - sums[...] * mean).astype(BF16)
            packed[a * degs : (a + 1) * degs, :chans] = centred[:degs]
            packed[a * degs : (a + 1) * degs, chans:] = centred[degs:]
        rest = jnp.concatenate([mean, spread], axis=1)
        lane = lax.broadcasted_iota(jnp.int32, (EXTRA, 2 * chans), 0)
        tail = jnp.zeros((EXTRA, 2 * chans), F32)
        for piece in range(PIECES):
            part = rest.astype(BF16).astype(F32)
            tail = jnp.where(lane == piece, part, tail)
            rest = rest - part
        packed[steps * degs :, :] = tail.astype(BF16)
        total = payload.shape[0]
        chunk = total // 2 if total <= 1024 else total // 8
        for start in range(0, total, chunk):
            pick = lax.broadcasted_iota(jnp.int32, (chunk, packed.shape[0]), 1)
            pick = (pick == column[start : start + chunk]).astype(F32).astype(BF16)
            payload[start : start + chunk] = dot(pick, packed[...]).astype(BF16)


def spread_kernel(legendre, place, out):
    slots, degs, nlat = legendre.shape
    total = out.shape[1]
    lat = lax.broadcasted_iota(jnp.int32, (nlat, total), 0)
    for j in range(slots):
        pick = (lat == place[j : j + 1]).astype(F32).astype(BF16)
        out[j * degs : (j + 1) * degs] = dot(legendre[j], pick).astype(BF16)


def spectral_kernel(
    lat_count, count, inv_root, lat_scale, mine, arrived, wide, mixing, gain, sums, back, norm, mixed
):
    total, lanes = arrived.shape
    chans = lanes // 2
    rows = total // lat_count
    slots = mixing.shape[0]
    degs = wide.shape[0] // slots
    data = arrived[...]
    pick_row = lax.broadcasted_iota(jnp.int32, (PIECES * lat_count, total), 0)
    pick_col = lax.broadcasted_iota(jnp.int32, (PIECES * lat_count, total), 1)
    base = rows - 4
    want = (pick_row % lat_count) * rows + base + pick_row // lat_count
    stats = dot((pick_col == want).astype(F32).astype(BF16), data)
    stats = stats.reshape(PIECES, lat_count, lanes)
    stats = stats[0] + (stats[1] + stats[2])
    means = stats[:, :chans]
    mean = jnp.sum(means, axis=0, keepdims=True) / lat_count
    offs = means - mean
    var = jnp.sum(stats[:, chans:] + count * offs * offs, axis=0, keepdims=True) / (
        count * lat_count
    )
    scale = gain[...] / jnp.sqrt(var + 1e-05)
    norm[0:1] = mean
    norm[1:2] = scale
    scale2 = jnp.concatenate([scale, scale], axis=1) * inv_root
    offs2 = jnp.concatenate([offs, offs], axis=1)
    full = data.astype(F32).reshape(lat_count, rows, lanes)
    full = (full + offs2[:, None, :] * sums[...][None]) * scale2[None]
    full = full.reshape(total, lanes).astype(BF16)
    degree = lax.broadcasted_iota(jnp.int32, (degs, lanes), 0)
    for j in range(slots):
        wave = mine[j]
        coef = dot(wide[j * degs : (j + 1) * degs], full)
        coef = jnp.where(degree >= wave, coef, 0.0).astype(BF16)
        re, im = coef[:, :chans], coef[:, chans:]
        w0, w1 = mixing[j, 0], mixing[j, 1]
        weight = jnp.where(wave == 0, 1.0, 2.0).astype(F32)
        out_re = (dot(re, w0) - dot(im, w1)).astype(BF16).astype(F32) * weight
        out_im = (dot(re, w1) + dot(im, w0)).astype(BF16).astype(F32) * weight
        mixed[j * degs : (j + 1) * degs, :chans] = out_re.astype(BF16)
        mixed[j * degs : (j + 1) * degs, chans:] = out_im.astype(BF16)
    back[...] = (dot(wide[...], mixed[...], ((0,), (0,))) * lat_scale).astype(BF16)


def inverse_kernel(inv_root, field, returned, column, table, norm, result, waves):
    lats, rows, chans = waves.shape
    degs = rows // 2
    total = returned.shape[0]

    @pl.when((pl.program_id(0) == 0) & (pl.program_id(1) == 0))
    def _():
        for a in range(lats):
            pick = lax.broadcasted_iota(jnp.int32, (degs, total), 0) + a * degs
            pick = (pick == column[...]).astype(F32).astype(BF16)
            value = dot(pick, returned[...]).astype(BF16)
            waves[a, :degs] = value[:, :chans]
            waves[a, degs:] = value[:, chans:]

    filtered = dot(table[...], waves[pl.program_id(0)]) * inv_root
    normed = ((field[0].astype(F32) - norm[0:1]) * norm[1:2]).astype(BF16).astype(F32)
    result[0] = (normed + filtered).astype(BF16)


def per_device(field, gain, slot_wave, legendre, mixing):
    lat_count = lax.axis_size("lat")
    lat_dev, width, chans = field.shape
    slot_dev, degs, nlat = legendre.shape
    lanes = 2 * chans
    data_rows = lat_dev * slot_dev
    rows = -(-(data_rows + PIECES + 1) // 8) * 8
    total = lat_count * rows
    inv_root = 1.0 / math.sqrt(width)
    table, sums = wave_tables(degs, width)
    whole = pl.BlockSpec(memory_space=pltpu.VMEM)

    waves = slot_wave.reshape(lat_count, slot_dev, 1)
    source = jnp.arange(lat_dev, dtype=jnp.int32)[None, None, :] * degs + waves
    source = jnp.where(waves < degs, source, -1).reshape(lat_count, data_rows)
    tail = np.full((lat_count, rows - data_rows), -1, np.int32)
    tail[:, rows - data_rows - 4 : rows - data_rows - 4 + PIECES] = lat_dev * degs + np.arange(PIECES)
    column = jnp.concatenate([source, jnp.asarray(tail)], axis=1)

    steps = lat_dev
    payload = pl.pallas_call(
        forward_kernel,
        grid=(steps,),
        in_specs=[
            pl.BlockSpec((1, width, chans), lambda i: (i, 0, 0)),
            pl.BlockSpec((2 * degs, width), lambda i: (0, 0)),
            pl.BlockSpec((2 * degs, 1), lambda i: (0, 0)),
            pl.BlockSpec((total, 1), lambda i: (0, 0)),
        ],
        out_specs=pl.BlockSpec((total, lanes), lambda i: (0, 0)),
        out_shape=jax.ShapeDtypeStruct((total, lanes), BF16),
        scratch_shapes=[
            pltpu.VMEM((steps, 2 * degs, chans), F32),
            pltpu.VMEM((steps * degs + EXTRA, lanes), BF16),
            pltpu.VMEM((8, chans), F32),
            pltpu.VMEM((2, 8, chans), F32),
        ],
        compiler_params=pltpu.CompilerParams(dimension_semantics=("arbitrary",)),
        name="forward",
    )(field, jnp.asarray(table), jnp.asarray(sums)[:, None], column.reshape(total, 1))
    arrived = lax.all_to_all(
        payload.reshape(lat_count, rows, lanes), "lat", split_axis=0, concat_axis=0, tiled=True
    ).reshape(total, lanes)

    place = np.full((slot_dev, lat_count, rows), -1, np.int32)
    for j in range(slot_dev):
        place[j, :, j * lat_dev : (j + 1) * lat_dev] = np.arange(nlat).reshape(lat_count, lat_dev)
    wide = pl.pallas_call(
        spread_kernel,
        in_specs=[whole, whole],
        out_specs=whole,
        out_shape=jax.ShapeDtypeStruct((slot_dev * degs, total), BF16),
        cost_estimate=pl.CostEstimate(
            flops=2 * slot_dev * degs * nlat * total, bytes_accessed=0, transcendentals=0
        ),
        name="spread",
    )(legendre, jnp.asarray(place.reshape(slot_dev, total)))

    mine = lax.dynamic_slice_in_dim(slot_wave, lax.axis_index("lat") * slot_dev, slot_dev, 0)
    pair = jnp.asarray(np.stack([sums[:degs], sums[degs:]]))
    known = jnp.where(mine < degs, pair[:, jnp.minimum(mine, degs - 1)], 0.0)
    known = jnp.repeat(known, lat_dev, axis=1)
    known = jnp.pad(known, ((0, 0), (0, rows - data_rows)))
    known = jnp.broadcast_to(known.T[:, :, None], (rows, 2, chans)).reshape(rows, lanes)
    back, norm = pl.pallas_call(
        functools.partial(
            spectral_kernel,
            lat_count,
            float(lat_dev * width),
            inv_root,
            math.sqrt(nlat / degs),
        ),
        in_specs=[pl.BlockSpec(memory_space=pltpu.SMEM)] + [whole] * 5,
        out_specs=(whole, whole),
        out_shape=(
            jax.ShapeDtypeStruct((total, lanes), BF16),
            jax.ShapeDtypeStruct((8, chans), F32),
        ),
        scratch_shapes=[pltpu.VMEM((slot_dev * degs, lanes), BF16)],
        name="spectral",
    )(mine, arrived, wide, mixing, gain[None], known)
    returned = lax.all_to_all(
        back.reshape(lat_count, rows, lanes), "lat", split_axis=0, concat_axis=0, tiled=True
    ).reshape(total, lanes)

    parts = 2
    return pl.pallas_call(
        functools.partial(inverse_kernel, inv_root),
        grid=(lat_dev, parts),
        in_specs=[
            pl.BlockSpec((1, width // parts, chans), lambda i, k: (i, k, 0)),
            pl.BlockSpec((total, lanes), lambda i, k: (0, 0)),
            pl.BlockSpec((1, total), lambda i, k: (0, 0)),
            pl.BlockSpec((width // parts, 2 * degs), lambda i, k: (k, 0)),
            pl.BlockSpec((8, chans), lambda i, k: (0, 0)),
        ],
        out_specs=pl.BlockSpec((1, width // parts, chans), lambda i, k: (i, k, 0)),
        out_shape=jax.ShapeDtypeStruct(field.shape, BF16),
        scratch_shapes=[pltpu.VMEM((lat_dev, 2 * degs, chans), BF16)],
        compiler_params=pltpu.CompilerParams(dimension_semantics=("arbitrary", "arbitrary")),
        name="inverse",
    )(field, returned, column.reshape(1, total), jnp.asarray(table.T.copy()), norm)


def solution(mesh):
    return jax.shard_map(
        per_device,
        mesh=mesh,
        in_specs=(
            P(("member", "lat"), None, None),
            P(),
            P(),
            P("lat", None, None),
            P("lat", None, None, None),
        ),
        out_specs=P(("member", "lat"), None, None),
        check_vma=False,
    )
```

```python
import functools
import math

import jax
import jax.numpy as jnp
import numpy as np
from jax import lax
from jax.experimental import pallas as pl
from jax.experimental.pallas import tpu as pltpu
from jax.sharding import PartitionSpec as P

F32 = jnp.float32
BF16 = jnp.bfloat16
PIECES = 3
EXTRA = 16


def dot(a, b, dims=((1,), (0,))):
    return lax.dot_general(a, b, (dims, ((), ())), preferred_element_type=F32)


def wave_tables(degs, width):
    turns = np.outer(np.arange(degs), np.arange(width)) % width
    phase = turns.astype(np.float64) * (2.0 * math.pi / width)
    table = np.concatenate([np.cos(phase), -np.sin(phase)]).astype(BF16)
    return table, table.astype(np.float64).sum(axis=1).astype(np.float32)


def slot_index(lookup, slot_wave, degs):
    depth = lookup.shape[1]
    slots = slot_wave.shape[1]
    lane = lax.broadcasted_iota(jnp.int32, (1, depth), 1)
    ends = jnp.where(lane == depth - 3, degs, jnp.where(lane == depth - 2, 1, -1))
    wave = jnp.concatenate(
        [jnp.where(slot_wave < degs, slot_wave, -16384), jnp.zeros((1, depth - slots), jnp.int32)],
        axis=1,
    )
    wave = jnp.broadcast_to(jnp.where(lane < slots, wave, ends), (128, depth))
    high = (wave >> 4).astype(F32).astype(BF16)
    low = (wave & 15).astype(F32).astype(BF16)
    nt = ((1,), (1,))
    return (dot(lookup, high, nt) * 16.0 + dot(lookup, low, nt)).astype(jnp.int32)


def forward_kernel(field, table, sums, waves, lookup, payload, packed, pick, shift, acc):
    step = pl.program_id(0)
    steps = pl.num_programs(0)
    rows, width = table.shape
    degs = rows // 2
    chans = field.shape[2]
    total, depth = pick.shape
    chunk = total // max(k for k in (1, 2, 4, 5) if total % (8 * k) == 0)
    opening = step == 0
    spec = dot(table[...], field[0])
    origin = jnp.where(opening, field[0, 0:16].astype(F32)[0:1], shift[1:2])
    total1 = jnp.where(opening, 0.0, acc[0])
    total2 = jnp.where(opening, 0.0, acc[1])
    part = width // max(k for k in range(1, 33) if width % (16 * k) == 0)
    for start in range(0, width, part):
        block = field[0, start : start + part]
        moved = block.astype(F32).reshape(part // 8, 8, chans) - origin
        total1 = total1 + jnp.sum(moved, axis=0)
        total2 = total2 + jnp.sum(moved * moved, axis=0)
    acc[0] = total1
    acc[1] = total2
    place = pl.ds(pl.multiple_of(jnp.minimum(step, total // chunk - 1) * chunk, chunk), chunk)
    index = slot_index(lookup[place], waves[...], degs)
    row = lax.broadcasted_iota(jnp.int32, (chunk, depth), 1)
    pick[place] = (row == index[:, 0:1]).astype(F32).astype(BF16)
    middle = jnp.where(opening, (spec[0:1] / width).astype(BF16).astype(F32), shift[0:1])
    shift[0:1] = middle
    shift[1:2] = origin
    centred = (spec - sums[...] * middle).astype(BF16)
    packed[pl.ds(step * degs, degs), :chans] = centred[:degs]
    packed[pl.ds(step * degs, degs), chans:] = centred[degs:]

    @pl.when(step == steps - 1)
    def _():
        count = float(width * (packed.shape[0] - EXTRA) // degs)
        delta = jnp.sum(acc[0], axis=0, keepdims=True) / count
        square = jnp.sum(acc[1], axis=0, keepdims=True)
        spread = jnp.maximum(square - count * delta * delta, 0.0)
        delta = (shift[1:2] - shift[0:1]) + delta
        lane = lax.broadcasted_iota(jnp.int32, (EXTRA, chans), 0)
        left = jnp.where(lane == 0, shift[0:1], 0.0)
        right = jnp.zeros((EXTRA, chans), F32)
        for piece in (1, 2):
            part = delta.astype(BF16).astype(F32)
            left = jnp.where(lane == piece, part, left)
            delta = delta - part
        for piece in range(PIECES):
            part = spread.astype(BF16).astype(F32)
            right = jnp.where(lane == piece, part, right)
            spread = spread - part
        packed[depth - EXTRA :, :chans] = left.astype(BF16)
        packed[depth - EXTRA :, chans:] = right.astype(BF16)
        payload[...] = dot(pick[...], packed[...]).astype(BF16)


def spread_kernel(legendre, place, out):
    slots, degs, nlat = legendre.shape
    total = out.shape[1]
    lat = lax.broadcasted_iota(jnp.int32, (nlat, total), 0)
    for j in range(slots):
        pick = (lat == place[j : j + 1]).astype(F32).astype(BF16)
        out[j * degs : (j + 1) * degs] = dot(legendre[j], pick).astype(BF16)


def unpack_kernel(degs, norm, waves, lookup, unpack):
    del norm
    total = unpack.shape[1]
    index = slot_index(lookup[...], waves[...], degs).T[0:1]
    for a in range(unpack.shape[0] // degs):
        row = lax.broadcasted_iota(jnp.int32, (degs, total), 0) + a * degs
        unpack[a * degs : (a + 1) * degs] = (row == index).astype(F32).astype(BF16)


def spectral_kernel(
    lat_count, count, inv_root, lat_scale, mine, arrived, wide, mixing, gain, sums, back, norm, mixed
):
    total, lanes = arrived.shape
    chans = lanes // 2
    rows = total // lat_count
    slots = mixing.shape[0]
    degs = wide.shape[0] // slots
    data = arrived[...]
    pick_row = lax.broadcasted_iota(jnp.int32, (PIECES * lat_count, total), 0)
    pick_col = lax.broadcasted_iota(jnp.int32, (PIECES * lat_count, total), 1)
    first = rows - 4
    want = (pick_row % lat_count) * rows + first + pick_row // lat_count
    stats = dot((pick_col == want).astype(F32).astype(BF16), data)
    stats = stats.reshape(PIECES, lat_count, lanes)
    shift = stats[0, :, :chans]
    delta = stats[1, :, :chans] + stats[2, :, :chans]
    spread = stats[0, :, chans:] + (stats[1, :, chans:] + stats[2, :, chans:])
    base = shift[0:1]
    drift = (shift - base) + delta
    drift_mean = jnp.sum(drift, axis=0, keepdims=True) / lat_count
    mean = base + drift_mean
    drift = drift - drift_mean
    var = jnp.sum(spread + count * drift * drift, axis=0, keepdims=True) / (count * lat_count)
    offs = (shift - base) - drift_mean
    scale = gain[...] / jnp.sqrt(var + 1e-05)
    norm[0:1] = mean
    norm[1:2] = scale
    scale2 = jnp.concatenate([scale, scale], axis=1) * inv_root
    offs2 = jnp.concatenate([offs, offs], axis=1)
    full = data.astype(F32).reshape(lat_count, rows, lanes)
    full = (full + offs2[:, None, :] * sums[...][None]) * scale2[None]
    full = full.reshape(total, lanes).astype(BF16)
    coefs = dot(wide[...], full)
    degree = lax.broadcasted_iota(jnp.int32, (degs, lanes), 0)
    for j in range(slots):
        wave = mine[j]
        coef = coefs[j * degs : (j + 1) * degs]
        coef = jnp.where(degree >= wave, coef, 0.0).astype(BF16)
        re, im = coef[:, :chans], coef[:, chans:]
        w0, w1 = mixing[j, 0], mixing[j, 1]
        weight = jnp.where(wave == 0, 1.0, 2.0).astype(F32)
        out_re = (dot(re, w0) - dot(im, w1)).astype(BF16).astype(F32) * weight
        out_im = (dot(re, w1) + dot(im, w0)).astype(BF16).astype(F32) * weight
        mixed[j * degs : (j + 1) * degs, :chans] = out_re.astype(BF16)
        mixed[j * degs : (j + 1) * degs, chans:] = out_im.astype(BF16)
    back[...] = (dot(wide[...], mixed[...], ((0,), (0,))) * (lat_scale * inv_root)).astype(BF16)


def inverse_kernel(field, returned, unpack, table, norm, result, coefs):
    lats, rows, chans = coefs.shape
    degs = rows // 2
    step, part = pl.program_id(0), pl.program_id(1)
    width = table.shape[0]

    @pl.when((step == 0) & (part == 0))
    def _():
        values = dot(unpack[...], returned[...]).astype(BF16)
        for a in range(lats):
            value = values[a * degs : (a + 1) * degs]
            coefs[a, :degs] = value[:, :chans]
            coefs[a, degs:] = value[:, chans:]

    span = result.shape[1]
    base = part * span
    mean, scale = norm[0:1], norm[1:2]
    waves = coefs[step]
    chunk = span // max(k for k in (1, 3) if span % (16 * k) == 0)
    for start in range(0, span, chunk):
        place = pl.ds(pl.multiple_of(base + start, 16), chunk)
        filtered = dot(table[place], waves)
        normed = (field[0, start : start + chunk].astype(F32) - mean) * scale
        result[0, start : start + chunk] = (normed + filtered).astype(BF16)


def per_device(field, gain, slot_wave, legendre, mixing):
    lat_count = lax.axis_size("lat")
    lat_dev, width, chans = field.shape
    slot_dev, degs, nlat = legendre.shape
    lanes = 2 * chans
    data_rows = lat_dev * slot_dev
    rows = -(-(data_rows + PIECES + 1) // 8) * 8
    total = lat_count * rows
    inv_root = 1.0 / math.sqrt(width)
    table, sums = wave_tables(degs, width)
    whole = pl.BlockSpec(memory_space=pltpu.VMEM)

    slots = lat_count * slot_dev
    deep = -(-(slots + 3) // 128) * 128
    lookup = np.zeros((lat_count, rows, deep), np.float32)
    for d in range(lat_count):
        for j in range(slot_dev):
            for a in range(lat_dev):
                lookup[d, j * lat_dev + a, d * slot_dev + j] = 1
                lookup[d, j * lat_dev + a, deep - 3] = a
    base = data_rows
    lookup[:, base : base + PIECES, deep - 3] = lat_dev
    lookup[:, base : base + PIECES, deep - 2] = np.arange(PIECES)
    lookup[:, base + PIECES :, deep - 1] = 1
    lookup = jnp.asarray(lookup.reshape(total, deep).astype(BF16))
    waves = slot_wave[None]

    steps = lat_dev
    depth = steps * degs + EXTRA
    limit = (16 if total <= 1024 else 60) * 2**20
    payload = pl.pallas_call(
        forward_kernel,
        grid=(steps,),
        in_specs=[
            pl.BlockSpec((1, width, chans), lambda i: (i, 0, 0)),
            pl.BlockSpec((2 * degs, width), lambda i: (0, 0)),
            pl.BlockSpec((2 * degs, 1), lambda i: (0, 0)),
            pl.BlockSpec((1, slots), lambda i: (0, 0)),
            pl.BlockSpec((total, deep), lambda i: (0, 0)),
        ],
        out_specs=whole,
        out_shape=jax.ShapeDtypeStruct((total, lanes), BF16),
        scratch_shapes=[
            pltpu.VMEM((depth, lanes), BF16),
            pltpu.VMEM((total, depth), BF16),
            pltpu.VMEM((8, chans), F32),
            pltpu.VMEM((2, 8, chans), F32),
        ],
        compiler_params=pltpu.CompilerParams(
            dimension_semantics=("arbitrary",),
            vmem_limit_bytes=max(limit, 56 * 2**20),
        ),
        name="forward",
    )(field, jnp.asarray(table), jnp.asarray(sums)[:, None], waves, lookup)
    arrived = lax.all_to_all(
        payload.reshape(lat_count, rows, lanes), "lat", split_axis=0, concat_axis=0, tiled=True
    ).reshape(total, lanes)

    place = np.full((slot_dev, lat_count, rows), -1, np.int32)
    for j in range(slot_dev):
        place[j, :, j * lat_dev : (j + 1) * lat_dev] = np.arange(nlat).reshape(lat_count, lat_dev)
    wide = pl.pallas_call(
        spread_kernel,
        in_specs=[whole] * 2,
        out_specs=whole,
        out_shape=jax.ShapeDtypeStruct((slot_dev * degs, total), BF16),
        cost_estimate=pl.CostEstimate(
            flops=2 * slot_dev * degs * nlat * total, bytes_accessed=0, transcendentals=0
        ),
        compiler_params=pltpu.CompilerParams(vmem_limit_bytes=limit),
        name="spread",
    )(legendre, jnp.asarray(place.reshape(slot_dev, total)))

    mine = lax.dynamic_slice_in_dim(slot_wave, lax.axis_index("lat") * slot_dev, slot_dev, 0)
    pair = jnp.asarray(np.stack([sums[:degs], sums[degs:]]))
    known = jnp.where(mine < degs, pair[:, jnp.minimum(mine, degs - 1)], 0.0)
    known = jnp.repeat(known, lat_dev, axis=1)
    known = jnp.pad(known, ((0, 0), (0, rows - data_rows)))
    known = jnp.broadcast_to(known.T[:, :, None], (rows, 2, chans)).reshape(rows, lanes)
    back, norm = pl.pallas_call(
        functools.partial(
            spectral_kernel,
            lat_count,
            float(lat_dev * width),
            inv_root,
            math.sqrt(nlat / degs),
        ),
        in_specs=[pl.BlockSpec(memory_space=pltpu.SMEM)] + [whole] * 5,
        out_specs=(whole, whole),
        out_shape=(
            jax.ShapeDtypeStruct((total, lanes), BF16),
            jax.ShapeDtypeStruct((8, chans), F32),
        ),
        scratch_shapes=[pltpu.VMEM((slot_dev * degs, lanes), BF16)],
        compiler_params=pltpu.CompilerParams(vmem_limit_bytes=limit),
        name="spectral",
    )(mine, arrived, wide, mixing, gain[None], known)
    unpack = pl.pallas_call(
        functools.partial(unpack_kernel, degs),
        in_specs=[whole] * 3,
        out_specs=whole,
        out_shape=jax.ShapeDtypeStruct((lat_dev * degs, total), BF16),
        cost_estimate=pl.CostEstimate(flops=10**9, bytes_accessed=0, transcendentals=0),
        compiler_params=pltpu.CompilerParams(vmem_limit_bytes=limit),
        name="unpack",
    )(norm, waves, lookup)
    returned = lax.all_to_all(
        back.reshape(lat_count, rows, lanes), "lat", split_axis=0, concat_axis=0, tiled=True
    ).reshape(total, lanes)

    parts = 1
    return pl.pallas_call(
        inverse_kernel,
        grid=(lat_dev, parts),
        in_specs=[pl.BlockSpec((1, width // parts, chans), lambda i, k: (i, k, 0))] + [whole] * 4,
        out_specs=pl.BlockSpec((1, width // parts, chans), lambda i, k: (i, k, 0)),
        out_shape=jax.ShapeDtypeStruct(field.shape, BF16),
        scratch_shapes=[pltpu.VMEM((lat_dev, 2 * degs, chans), BF16)],
        compiler_params=pltpu.CompilerParams(
            dimension_semantics=("arbitrary", "arbitrary"), vmem_limit_bytes=60 * 2**20
        ),
        name="inverse",
    )(field, returned, unpack, jnp.asarray(table.T.copy()), norm)


def solution(mesh):
    return jax.shard_map(
        per_device,
        mesh=mesh,
        in_specs=(
            P(("member", "lat"), None, None),
            P(),
            P(),
            P("lat", None, None),
            P("lat", None, None, None),
        ),
        out_specs=P(("member", "lat"), None, None),
        check_vma=False,
    )
```
